32 devices in a mesh: parts: 2 (over y), mkt: 8 (over z, x), draw: 2 (over core).
Axes of the slice: x: 2, y: 2, z: 4, core: 2. Of those that a mesh axis runs over, the one named last changes fastest.
Arguments:
- characters: float32 [128, 6, 128], P(('parts', 'mkt')), parts along dimension 0, may hold values from -3 to 3
- taste_draws: float32 [128, 6, 4096], P(('parts', 'mkt'), None, 'draw'), parts along dimension 0, may hold values from -3 to 3
- prices: float32 [128, 128], P(('parts', 'mkt')), parts along dimension 0, may hold values from 0.5 to 2
- obs_shares: float32 [128, 128], P(('parts', 'mkt')), parts along dimension 0, may hold values from 0 to 1, as said below
- firm_ids: int32 [128, 128], P(('parts', 'mkt')), parts along dimension 0, may hold values from 0 to 7
- owner_step: int32 [128, 1], P(('parts', 'mkt')), parts along dimension 0, may hold values from 0 to 7; in each aligned block of 8 rows (0 to 7, 8 to 15, ...) at most 4 rows name the same one
- spread_coefs: float32 [6], replicated, may hold values from 0.2 to 0.6
- price_params: float32 [2], replicated, may hold values from 0 to 0.5
Outputs:
- mean_util: float32 [128, 128], P(('parts', 'mkt', 'draw')), parts along dimension 0
- markups: float32 [16, 8, 4, 128], P(('parts', 'mkt'), None, 'draw'), parts along dimension 0
The draws below stay inside these ranges and needn't reach their ends.
There are 2 independent parts, one for each index of `parts`. The reference program is written for one: setup_inputs(seed, part) draws one part's arguments, and reference() takes and returns one part's arrays. A program takes and returns all parts, laid end to end along the dimension named above; an argument that names none is the same for every part. Nothing has to cross between parts.
Inputs may be any that keep to these rules, and one draw needn't show every extreme that they name: `owner_step`: among the markets of one index of mkt, no value occurs more than 4 times, and in every draw some value occurs exactly 4 times among the markets of some device. `obs_shares`: every entry is positive, and each row sums to between 2/3 and 4/5.
All inputs are finite; a program needn't handle non-finite values.
Results may differ from the reference program's by a relative error of at most 0.0003.
Values sent between devices are 32-bit elements; how exact they have to be, the bound alone decides.
A program may use at most 64 MiB of HBM per device.

```python
import math
import jax
import jax.numpy as jnp
import numpy as np
from jax import lax

J = 128
K = 6
FIRMS = 8
ITERS = 4
MK_DEV = 8
W = 8
CAP = 4
R = 4096
MARKETS = 64
N_MKT = 8


def draw_obs_shares(key, part):
    first, second = jax.random.split(jax.random.fold_in(key, 11))
    weights = jnp.exp(jax.random.uniform(first, (MARKETS, J), jnp.float32, -1.0, 1.0))
    ratio = jax.random.uniform(second, (MARKETS, 1), jnp.float32, 0.25, 0.5)
    total = jnp.sum(weights, axis=1, keepdims=True)
    return weights / (total * (1.0 + ratio))


def with_ends(values, own_key, least, largest):
    extent = values.shape
    index_at = [jax.random.randint(jax.random.fold_in(own_key, axis), (), 0, extent[axis]) for axis in range(len(extent))]
    values = values.at[tuple(index_at)].set(least)
    longest = extent.index(max(extent))
    index_at[longest] = (index_at[longest] + 1) % extent[longest]
    return values.at[tuple(index_at)].set(largest)


def levels(stream_key, extent, pieces, least, largest):
    def one(position, blocks):
        steps = jax.random.uniform(jax.random.fold_in(jax.random.fold_in(stream_key, 6), position), (blocks,), jnp.float32, least / len(pieces), largest / len(pieces))
        return jnp.repeat(jnp.exp(steps), extent[position] // blocks).reshape((-1,) + (1,) * (len(extent) - position - 1))

    factor_of = one(*pieces[0])
    for cut in pieces[1:]:
        factor_of = factor_of * one(*cut)
    return factor_of


def assign_block(own_key, own, number, rows, amount, top, limit, skew):
    ranking = jax.random.permutation(own_key, amount)
    packed, usual = portions_of(amount, rows * top, limit, skew, True), portions_of(amount, rows * top, limit, skew, False)
    places = jnp.arange(amount)

    def named(sizes, offset_by):
        used = int((sizes > 0).sum())
        fixed = max(1, used // 4)
        moved = fixed + (places - fixed + offset_by * (used - fixed)) % max(1, amount - fixed)
        return jnp.zeros((amount,), jnp.int32).at[ranking[jnp.where(places < fixed, places, moved)]].set(jnp.asarray(sizes, jnp.int32))

    sizes = jnp.where(number % 4 == 0, named(packed, number // 4), named(usual, number - number // 4 - 1))
    mixed = jax.random.permutation(jax.random.fold_in(own, 3), amount)
    giver, sink = mixed[0:amount // 2 * 2:2], mixed[1:amount // 2 * 2:2]
    room = jnp.minimum(sizes[giver] - 1, limit - sizes[sink]) // 2
    room = jnp.where((giver == ranking[0]) | (sink == ranking[0]) | (sizes[sink] == 0), 0, jnp.maximum(room, 0))
    moved = jax.random.randint(jax.random.fold_in(own, 4), (amount // 2,), 0, 1 << 20) % (room + 1)
    sizes = sizes.at[giver].add(-moved).at[sink].add(moved)
    items = jnp.searchsorted(jnp.cumsum(sizes), jnp.arange(rows * top), side="right").astype(jnp.int32)
    grid = items.reshape(top, rows).T
    grid = grid[jax.random.permutation(jax.random.fold_in(own, 1), rows)]
    offset_by = jax.random.randint(jax.random.fold_in(own, 2), (rows, 1), 0, top)
    return jnp.take_along_axis(grid, (jnp.arange(top)[None, :] + offset_by) % top, axis=1)


def portions_of(number_of, total, limit, skew, full):
    weights = [(1 << 20) // math.isqrt(grade ** skew) + 1 for grade in range(1, number_of + 1)]
    largest = limit if full else min(limit, max(-(-total // number_of), total * weights[0] // sum(weights)))
    least = 1 if total - largest >= number_of - 1 else 0
    holding, spare = [largest] + [least] * (number_of - 1), total - largest - least * (number_of - 1)
    while spare > 0:
        movable = [i for i in range(1, number_of) if holding[i] < largest] or [i for i in range(1, number_of) if holding[i] < limit]
        pool, remaining = sum([weights[i] for i in movable]), spare
        for i in movable:
            extra = min(limit - holding[i], max(1, remaining * weights[i] // pool), spare)
            holding[i] = holding[i] + extra
            spare = spare - extra
    return np.array(holding)


def normal_values(rng, shape, scale, reach, cuts=(), held_as=jnp.bfloat16):
    gain = levels(rng, shape, cuts, -0.22, 0.18) if cuts else 1.0
    drawn = jax.random.normal(rng, shape, jnp.float32) * scale * gain
    return jnp.minimum(jnp.maximum(drawn, -reach), reach).astype(held_as)


def setup_inputs(seed: int = 0, part: int = 0) -> dict:
    keys = jax.random.split(jax.random.key(seed), 9)
    part_splits = jax.random.split(jax.random.fold_in(keys[8], part), 9)
    characters = normal_values(part_splits[0], (MARKETS, K, J), 1.0, 3.0, ((0, 8),), jnp.float32)
    taste_draws = normal_values(part_splits[1], (MARKETS, K, R), 1.0, 3.0, ((0, 8), (2, 2)), jnp.float32)
    prices = jnp.clip(jnp.exp(math.log(2.0) - 1.3862944 * jax.random.uniform(part_splits[2], (MARKETS, J), jnp.float32) ** levels(part_splits[2], (MARKETS, J), ((0, 8),), -0.2, 0.2)), 0.5, 2.0)
    obs_shares = draw_obs_shares(jax.random.fold_in(jax.random.fold_in(keys[8], part), 71), part)
    firm_ids = with_ends(jax.random.randint(part_splits[4], (MARKETS, J), 0, FIRMS), jax.random.fold_in(part_splits[4], 1), 0, FIRMS - 1).astype(jnp.int32)
    owner_step_keys = jax.random.split(jax.random.fold_in(part_splits[5], 1), MARKETS // MK_DEV)
    owner_step_turns = jax.random.permutation(jax.random.fold_in(part_splits[5], 3), MARKETS // MK_DEV)
    owner_step = jax.vmap(lambda own, number: assign_block(jax.random.fold_in(part_splits[5], 2), own, number, MK_DEV, W, 1, CAP, 2))(owner_step_keys, owner_step_turns).reshape((MARKETS, 1))
    spread_coefs = jnp.clip(jnp.exp(jax.random.uniform(keys[6], (K,), jnp.float32, math.log(0.2), math.log(0.6))), 0.2, 0.6)
    price_params = jnp.clip(jax.random.uniform(keys[7], (2,), jnp.float32, 0.0, 0.5), 0.0, 0.5)
    return {"characters": characters, "taste_draws": taste_draws, "prices": prices, "obs_shares": obs_shares, "firm_ids": firm_ids, "owner_step": owner_step, "spread_coefs": spread_coefs, "price_params": price_params}


HIGH = lax.Precision.HIGHEST

def utilities(characters, taste_draws, prices, spread_coefs, price_params):
    sensitivity = jnp.exp(price_params[0] + price_params[1] * taste_draws[0])
    loadings = characters * spread_coefs[:, None]
    spread = jnp.dot(loadings.T.astype(jnp.float32), taste_draws.astype(jnp.float32), precision=HIGH, preferred_element_type=jnp.float32)
    spread = spread - prices[:, None] * sensitivity[None, :]
    return (spread, sensitivity)

def purchase(mean_value, spread):
    exp_util = jnp.exp(mean_value[:, None] + spread)
    return exp_util / (1.0 + jnp.sum(exp_util, axis=0, keepdims=True))

def jacobian_of(purchase_prob, sensitivity, firm_ids, draw_count):
    own_slope = jnp.dot(purchase_prob.astype(jnp.float32), sensitivity.astype(jnp.float32), precision=HIGH, preferred_element_type=jnp.float32) / draw_count
    cross_term = jnp.dot((purchase_prob * sensitivity[None, :]).astype(jnp.float32), purchase_prob.T.astype(jnp.float32), precision=HIGH, preferred_element_type=jnp.float32) / draw_count
    same_firm = (firm_ids[:, None] == firm_ids[None, :]).astype(jnp.float32)
    return same_firm * (jnp.diag(own_slope) - cross_term)

def slot_ranks(offsets, per_device):
    grouped = offsets.reshape(-1, per_device)
    places = jnp.arange(per_device, dtype=jnp.int32)
    earlier = places[None, :] < places[:, None]
    match = grouped[:, :, None] == grouped[:, None, :]
    return jnp.sum(jnp.logical_and(match, earlier[None]), axis=2).astype(jnp.int32).reshape(-1)

def reference(characters, taste_draws, prices, obs_shares, firm_ids, owner_step, spread_coefs, price_params):

    def per_market(inputs):
        market_chars, market_taste, market_prices, market_obs, market_firms = inputs
        spread, sensitivity = utilities(market_chars, market_taste, market_prices, spread_coefs, price_params)
        mean_value = jnp.log(market_obs) - jnp.log(1.0 - jnp.sum(market_obs))
        for turn in range(ITERS):
            shares = jnp.sum(purchase(mean_value, spread), axis=1) / R
            mean_value = mean_value + jnp.log(market_obs) - jnp.log(shares)
        jacobian = jacobian_of(purchase(mean_value, spread), sensitivity, market_firms, R)
        return (mean_value, jnp.linalg.solve(jacobian, market_obs))
    mean_util, solved = lax.map(per_market, (characters, taste_draws, prices, obs_shares, firm_ids))
    offsets = owner_step[:, 0].astype(jnp.int32)
    market_index = jnp.arange(MARKETS, dtype=jnp.int32)
    source = market_index // MK_DEV
    ranks = slot_ranks(offsets, MK_DEV)
    owner = (source + offsets) % N_MKT
    markups = jnp.zeros((N_MKT, W, CAP, J), jnp.float32).at[owner, offsets, ranks].set(solved)
    return (mean_util, markups)
```

```python
import functools

import jax
import jax.numpy as jnp
from jax import lax
from jax.experimental import pallas as pl
from jax.experimental.pallas import tpu as pltpu
from jax.sharding import PartitionSpec as P

ITERS = 4
CAPC = 2
W = 8
LOG2E = 1.4426950408889634
LN2 = 0.6931471805599453
SWEEPS = 6
DOUBLINGS = 26
TOL = 3e-7
MESH = pl.DeviceIdType.MESH
HIGH = lax.Precision.HIGHEST
F32 = jnp.float32
BF16 = jnp.bfloat16


def exchange_kernel(taste_ref, out_ref, send_sem, recv_sem):
    core = lax.axis_index("draw")
    half = out_ref.shape[0]
    barrier = pltpu.get_barrier_semaphore()
    pl.semaphore_signal(barrier, inc=1, device_id={"draw": 1 - core}, device_id_type=MESH)
    pl.semaphore_wait(barrier, 1)
    copy = pltpu.make_async_remote_copy(
        src_ref=taste_ref.at[pl.ds((1 - core) * half, half)],
        dst_ref=out_ref,
        send_sem=send_sem,
        recv_sem=recv_sem,
        device_id={"draw": 1 - core},
        device_id_type=MESH,
    )
    copy.start()
    copy.wait()


def exchange(taste_draws):
    half = taste_draws.shape[0] // 2
    return pl.pallas_call(
        exchange_kernel,
        out_shape=jax.ShapeDtypeStruct((half,) + taste_draws.shape[1:], F32),
        in_specs=[pl.BlockSpec(memory_space=pl.ANY)],
        out_specs=pl.BlockSpec(memory_space=pl.ANY),
        scratch_shapes=[pltpu.SemaphoreType.DMA, pltpu.SemaphoreType.DMA],
        compiler_params=pltpu.CompilerParams(collective_id=0, has_side_effects=True),
        name="exchange",
    )(taste_draws)


def split3(value):
    high = value.astype(BF16).astype(F32)
    rest = value - high
    middle = rest.astype(BF16).astype(F32)
    return high, middle, rest - middle


def market_kernel(
    coef_ref, params_ref, steps_ref, chars_ref, taste_ref, other_ref, prices_ref, obs_ref,
    firms_ref, util_ref, placed_ref,
    e_ref, q_ref, left_ref, right_ref, stack_ref, root_ref, v_ref, n_ref, m_ref,
):
    core = lax.axis_index("draw")
    here, terms, width = chars_ref.shape
    half = here // 2
    part = taste_ref.shape[2]
    total = 2 * part
    lanes = 128
    chunks = total // lanes
    first = core * half

    row_i = lax.broadcasted_iota(jnp.int32, (width, width), 0)
    col_i = lax.broadcasted_iota(jnp.int32, (width, width), 1)
    eye = (row_i == col_i).astype(F32)

    obs_rows = [obs_ref[pl.ds(first + i, 1), :] for i in range(half)]
    firm_rows = [firms_ref[pl.ds(first + i, 1), :].astype(F32) for i in range(half)]
    rows = jnp.zeros((width, width), F32)
    for i in range(half):
        rows = jnp.where(row_i == i, obs_rows[i], rows)
        rows = jnp.where(row_i == half + i, firm_rows[i], rows)
    cols = rows.T

    finals = jnp.zeros((width, width), F32)
    for i in range(half):
        obs_row = obs_rows[i]
        obs_col = cols[:, i:i + 1]
        left_ref[...] = jnp.zeros_like(left_ref)
        for k in range(terms):
            left_ref[k:k + 1, :] = chars_ref[first + i, k:k + 1, :] * coef_ref[k] * LOG2E
        left_ref[terms:terms + 1, :] = prices_ref[pl.ds(first + i, 1), :] * (-LOG2E)
        lh, lm, ll = split3(left_ref[...])
        left = jnp.concatenate([lh, lh, lm, lm, lh, ll], axis=0).T.astype(BF16)
        right_ref[...] = jnp.zeros_like(right_ref)
        for h in range(2):
            taste = taste_ref[first + i] if h == 0 else other_ref[i]
            log_sens = (params_ref[0] + params_ref[1] * taste[0:1, :]) * LOG2E
            right_ref[0:terms, h * part:(h + 1) * part] = taste
            right_ref[terms:terms + 1, h * part:(h + 1) * part] = jnp.exp2(log_sens)
            root_ref[0:1, h * part:(h + 1) * part] = jnp.exp2(0.5 * log_sens)
        xh, xm, xl = split3(right_ref[...])
        stack_ref[...] = jnp.concatenate([xh, xm, xh, xm, xl, xh], axis=0).astype(BF16)

        wide = 4 * lanes

        def spread_chunk(c, top):
            at = pl.ds(pl.multiple_of(c * wide, wide), wide)
            s = jnp.dot(left, stack_ref[:, at], preferred_element_type=F32)
            e_ref[i, :, at] = s
            for b in range(4):
                top = jnp.maximum(top, s[:, b * lanes:(b + 1) * lanes])
            return top

        top = lax.fori_loop(
            0, total // wide, spread_chunk, jnp.full((width, lanes), -jnp.inf, F32), unroll=2
        )
        top = jnp.max(top, axis=1, keepdims=True)
        outside = 1.0 - jnp.sum(obs_row, axis=1, keepdims=True)
        start = (jnp.log(obs_col) - jnp.log(outside)) * LOG2E + top
        v_ref[...] = jnp.broadcast_to(jnp.exp2(start), (width, lanes))
        m_ref[...] = jnp.broadcast_to(top, (width, lanes))

        def first_chunk(c, acc):
            at = pl.ds(pl.multiple_of(c * lanes, lanes), lanes)
            e = jnp.exp2(e_ref[i, :, at] - m_ref[...])
            e_ref[i, :, at] = e
            inv = 1.0 / (1.0 + jnp.sum(e * v_ref[...], axis=0, keepdims=True))
            return acc + e * inv

        def next_chunk(c, acc):
            at = pl.ds(pl.multiple_of(c * lanes, lanes), lanes)
            e = e_ref[i, :, at]
            inv = 1.0 / (1.0 + jnp.sum(e * v_ref[...], axis=0, keepdims=True))
            return acc + e * inv

        for turn in range(ITERS):
            acc = lax.fori_loop(
                0, chunks, first_chunk if turn == 0 else next_chunk,
                jnp.zeros((width, lanes), F32), unroll=4,
            )
            share = jnp.sum(acc, axis=1, keepdims=True) * (1.0 / total)
            v_ref[...] = jnp.broadcast_to(obs_col / share, (width, lanes))
        mean = jnp.log(obs_col) - jnp.log(share) - top * LN2
        finals = jnp.where(col_i == i, mean, finals)

        def last_chunk(c, acc):
            at = pl.ds(pl.multiple_of(c * lanes, lanes), lanes)
            ve = e_ref[i, :, at] * v_ref[...]
            inv = 1.0 / (1.0 + jnp.sum(ve, axis=0, keepdims=True))
            root = root_ref[0:1, at]
            q = ve * (inv * root)
            high = q.astype(BF16)
            q_ref[0:width, at] = high
            q_ref[width:2 * width, at] = (q - high.astype(F32)).astype(BF16)
            return acc + q * root

        own = lax.fori_loop(0, chunks, last_chunk, jnp.zeros((width, lanes), F32), unroll=4)
        own = jnp.sum(own, axis=1, keepdims=True)
        both = lax.dot_general(
            q_ref[...], q_ref[...], (((1,), (1,)), ((), ())), preferred_element_type=F32
        )
        cross = both[0:width, 0:width] + (both[0:width, width:] + both[width:, 0:width])
        same = cols[:, half + i:half + i + 1] == firm_rows[i]
        n_ref[i] = jnp.where(same, eye * own - cross, 0.0) * (1.0 / total)

    util_ref[...] = finals.T[0:half, :]

    scales, c_rows, c_cols, y_rows, y_cols = [], [], [], [], []
    for i in range(half):
        jac = n_ref[i]
        diag = jac * eye
        s_row = lax.rsqrt(jnp.sum(diag, axis=0, keepdims=True))
        s_col = lax.rsqrt(jnp.sum(diag, axis=1, keepdims=True))
        n_ref[i] = eye - s_col * jac * s_row
        scales.append(s_row)
        c_rows.append(s_row * obs_rows[i])
        c_cols.append(s_col * cols[:, i:i + 1])
    y_rows = tuple(c_rows)

    def sweep(_, ys):
        out = []
        for i in range(half):
            y_col = c_cols[i] + jnp.sum(n_ref[i] * ys[i], axis=1, keepdims=True)
            out.append(c_rows[i] + jnp.sum(n_ref[i] * y_col, axis=0, keepdims=True))
        return tuple(out)

    y_rows = lax.fori_loop(0, SWEEPS, sweep, y_rows)
    rests = []
    for i in range(half):
        n_col = jnp.sum(n_ref[i] * y_rows[i], axis=1, keepdims=True)
        n_row = jnp.sum(eye * n_col, axis=0, keepdims=True)
        rests.append(c_rows[i] + n_row - y_rows[i])

    def size_of(vectors, against):
        worst = jnp.zeros((1, 1), F32)
        for i in range(half):
            top = jnp.max(jnp.abs(vectors[i]), axis=1, keepdims=True)
            worst = jnp.maximum(worst, top / jnp.max(jnp.abs(against[i]), axis=1, keepdims=True))
        return jnp.max(worst)

    def again(state):
        return jnp.logical_and(state[0] < DOUBLINGS, state[1] > TOL)

    def double(state):
        step, _, errors = state
        added, fresh = [], []
        for i in range(half):
            power = n_ref[i]
            eight = jnp.broadcast_to(errors[i], (8, width))
            more = jnp.dot(eight, power, precision=HIGH, preferred_element_type=F32)[0:1, :]
            added.append(more)
            fresh.append(errors[i] + more)
            n_ref[i] = jnp.dot(power, power, precision=HIGH, preferred_element_type=F32)
        return step + 1, size_of(added, y_rows), tuple(fresh)

    state = lax.while_loop(again, double, (0, size_of(rests, y_rows), tuple(rests)))
    out_row = lax.broadcasted_iota(jnp.int32, placed_ref.shape, 0)
    placed = jnp.zeros(placed_ref.shape, F32)
    for i in range(half):
        x = scales[i] * (y_rows[i] + state[2][i])
        mine = steps_ref[first + i]
        rank = 0
        for other in range(here):
            hit = jnp.logical_and(steps_ref[other] == mine, other < first + i)
            rank = rank + hit.astype(jnp.int32)
        upper = (rank >= CAPC).astype(jnp.int32)
        at = upper * (W * CAPC) + mine * CAPC + (rank - upper * CAPC)
        placed = jnp.where(out_row == at, x, placed)
    placed_ref[...] = placed


def solve_markets(coefs, params, steps, chars, taste, other, prices, obs, firms):
    here, terms, width = chars.shape
    half = here // 2
    total = 2 * taste.shape[2]
    smem = pl.BlockSpec(memory_space=pltpu.SMEM)
    vmem = pl.BlockSpec(memory_space=pltpu.VMEM)
    padded = -(-(terms + 1) // 8) * 8
    return pl.pallas_call(
        market_kernel,
        out_shape=(
            jax.ShapeDtypeStruct((half, width), F32),
            jax.ShapeDtypeStruct((2 * W * CAPC, width), F32),
        ),
        in_specs=[smem] * 3 + [vmem] * 6,
        out_specs=(vmem, vmem),
        scratch_shapes=[
            pltpu.VMEM((half, width, total), F32),
            pltpu.VMEM((2 * width, total), BF16),
            pltpu.VMEM((padded, width), F32),
            pltpu.VMEM((padded, total), F32),
            pltpu.VMEM((6 * padded, total), BF16),
            pltpu.VMEM((8, total), F32),
            pltpu.VMEM((width, 128), F32),
            pltpu.VMEM((half, width, width), F32),
            pltpu.VMEM((width, 128), F32),
        ],
        name="markets",
    )(coefs, params, steps, chars, taste, other, prices, obs, firms)


def route_kernel(markets, placed_ref, out_ref, got_ref, send_sem, recv_sem):
    core = lax.axis_index("draw")
    me = lax.axis_index("mkt")
    pairs = [(w, flip) for w in range(W) for flip in range(2) if (w, flip) != (0, 0)]
    barrier = pltpu.get_barrier_semaphore()

    def peer(step, flip):
        to_core = core if flip == 0 else 1 - core
        return {"mkt": lax.rem(me + step + markets, markets), "draw": to_core}

    for w, flip in pairs:
        pl.semaphore_signal(barrier, inc=1, device_id=peer(-w, flip), device_id_type=MESH)
    pl.semaphore_wait(barrier, len(pairs))
    copies = []
    for w, flip in pairs:
        to_core = core if flip == 0 else 1 - core
        copy = pltpu.make_async_remote_copy(
            src_ref=placed_ref.at[to_core, w],
            dst_ref=got_ref.at[flip, w],
            send_sem=send_sem.at[flip, w],
            recv_sem=recv_sem.at[flip, w],
            device_id=peer(w, flip),
            device_id_type=MESH,
        )
        copy.start()
        copies.append(copy)
    for copy in copies:
        copy.wait()
    out_ref[0, 0] = placed_ref[core, 0] + got_ref[1, 0]
    for w in range(1, W):
        out_ref[0, w] = got_ref[0, w] + got_ref[1, w]


def route(markets, placed):
    width = placed.shape[-1]
    vmem = pl.BlockSpec(memory_space=pltpu.VMEM)
    return pl.pallas_call(
        functools.partial(route_kernel, markets),
        out_shape=jax.ShapeDtypeStruct((1, W, CAPC, width), F32),
        in_specs=[vmem],
        out_specs=vmem,
        scratch_shapes=[
            pltpu.VMEM((2, W, CAPC, width), F32),
            pltpu.SemaphoreType.DMA((2, W)),
            pltpu.SemaphoreType.DMA((2, W)),
        ],
        compiler_params=pltpu.CompilerParams(collective_id=1, has_side_effects=True),
        name="route",
    )(placed.reshape(2, W, CAPC, width))


def body(
    markets,
    characters, taste_draws, prices, obs_shares, firm_ids, owner_step, spread_coefs, price_params,
):
    other = exchange(taste_draws)
    mean_util, placed = solve_markets(
        spread_coefs, price_params, owner_step[:, 0], characters, taste_draws, other,
        prices, obs_shares, firm_ids,
    )
    return mean_util, route(markets, placed)


def solution(mesh):
    placed = (
        P(("parts", "mkt"), None, None),
        P(("parts", "mkt"), None, "draw"),
        P(("parts", "mkt"), None),
        P(("parts", "mkt"), None),
        P(("parts", "mkt"), None),
        P(("parts", "mkt"), None),
        P(),
        P(),
    )
    return jax.shard_map(
        functools.partial(body, mesh.shape["mkt"]),
        mesh=mesh,
        in_specs=placed,
        out_specs=(P(("parts", "mkt", "draw"), None), P(("parts", "mkt"), None, "draw", None)),
        check_vma=False,
    )
```

```python
import functools

import jax
import jax.numpy as jnp
from jax import lax
from jax.experimental import pallas as pl
from jax.experimental.pallas import tpu as pltpu
from jax.sharding import PartitionSpec as P

ITERS = 4
CAPC = 2
W = 8
LOG2E = 1.4426950408889634
LN2 = 0.6931471805599453
SWEEPS = 6
U_SPREAD = 8
U_FIRST = 32
U_NEXT = 32
U_LAST = 32
DOUBLINGS = 26
TOL = 3e-7
MESH = pl.DeviceIdType.MESH
HIGH = lax.Precision.HIGHEST
F32 = jnp.float32
BF16 = jnp.bfloat16


def exchange_kernel(taste_ref, out_ref, send_sem, recv_sem):
    core = lax.axis_index("draw")
    barrier = pltpu.get_barrier_semaphore()
    pl.semaphore_signal(barrier, inc=1, device_id={"draw": 1 - core}, device_id_type=MESH)
    pl.semaphore_wait(barrier, 1)
    copy = pltpu.make_async_remote_copy(
        src_ref=taste_ref,
        dst_ref=out_ref,
        send_sem=send_sem,
        recv_sem=recv_sem,
        device_id={"draw": 1 - core},
        device_id_type=MESH,
    )
    copy.start()
    copy.wait()


def exchange(taste_draws):
    return pl.pallas_call(
        exchange_kernel,
        out_shape=jax.ShapeDtypeStruct(taste_draws.shape, F32),
        in_specs=[pl.BlockSpec(memory_space=pl.ANY)],
        out_specs=pl.BlockSpec(memory_space=pl.ANY),
        scratch_shapes=[pltpu.SemaphoreType.DMA, pltpu.SemaphoreType.DMA],
        compiler_params=pltpu.CompilerParams(collective_id=0, has_side_effects=True),
        name="exchange",
    )(taste_draws)


def split3(value):
    high = value.astype(BF16).astype(F32)
    rest = value - high
    middle = rest.astype(BF16).astype(F32)
    return high, middle, rest - middle


def market_kernel(
    coef_ref, params_ref, steps_ref, chars_ref, taste_ref, other_ref, prices_ref, obs_ref,
    firms_ref, util_ref, placed_ref,
    e_ref, q_ref, left_ref, right_ref, stack_ref, root_ref, v_ref, n_ref, m_ref, b_ref, f_ref,
    inv_ref,
):
    core = lax.axis_index("draw")
    terms, here, width = chars_ref.shape
    half = here // 2
    part = taste_ref.shape[2]
    total = 2 * part
    lanes = 128
    chunks = total // lanes
    first = core * half

    row_i = lax.broadcasted_iota(jnp.int32, (width, width), 0)
    col_i = lax.broadcasted_iota(jnp.int32, (width, width), 1)
    eye = (row_i == col_i).astype(F32)

    obs_rows = [obs_ref[pl.ds(first + i, 1), :] for i in range(half)]
    rows = jnp.zeros((width, width), F32)
    for i in range(half):
        rows = jnp.where(row_i == i, obs_rows[i], rows)
        firm_row = firms_ref[pl.ds(first + i, 1), :].astype(F32)
        rows = jnp.where(row_i == half + i, firm_row, rows)
    cols = rows.T
    for i in range(half):
        b_ref[i] = jnp.broadcast_to(cols[:, i:i + 1], (width, lanes))
        f_ref[i] = jnp.broadcast_to(cols[:, half + i:half + i + 1], (width, lanes))
    left_ref[...] = jnp.zeros_like(left_ref)
    right_ref[...] = jnp.zeros_like(right_ref)

    def market(i, finals):
        m = first + i
        obs_row = obs_ref[pl.ds(m, 1), :]
        obs_col = b_ref[i]
        for k in range(terms):
            left_ref[k:k + 1, :] = chars_ref[k, pl.ds(m, 1), :] * coef_ref[k] * LOG2E
        left_ref[terms:terms + 1, :] = prices_ref[pl.ds(m, 1), :] * (-LOG2E)
        lh, lm, ll = split3(left_ref[...])
        left = jnp.concatenate([lh, lh, lm, lm, lh, ll], axis=0).T.astype(BF16)
        for h, source in enumerate((taste_ref, other_ref)):
            at = slice(h * part, (h + 1) * part)
            for k in range(terms):
                right_ref[k:k + 1, at] = source[k, pl.ds(m, 1), :]
            log_sens = (params_ref[0] + params_ref[1] * right_ref[0:1, at]) * LOG2E
            root = jnp.exp2(0.5 * log_sens)
            root_ref[0:1, at] = root
            right_ref[terms:terms + 1, at] = jnp.exp2(log_sens)
        xh, xm, xl = split3(right_ref[...])
        stack_ref[...] = jnp.concatenate([xh, xm, xh, xm, xl, xh], axis=0).astype(BF16)

        wide = 4 * lanes

        def spread_chunk(c, top):
            at = pl.ds(pl.multiple_of(c * wide, wide), wide)
            s = jnp.dot(left, stack_ref[:, at], preferred_element_type=F32)
            e_ref[i, :, at] = s
            for b in range(4):
                top = jnp.maximum(top, s[:, b * lanes:(b + 1) * lanes])
            return top

        top = lax.fori_loop(
            0, total // wide, spread_chunk, jnp.full((width, lanes), -jnp.inf, F32),
            unroll=U_SPREAD,
        )
        top = jnp.max(top, axis=1, keepdims=True)
        outside = 1.0 - jnp.sum(obs_row, axis=1, keepdims=True)
        start = (jnp.log(obs_col) - jnp.log(outside)) * LOG2E + top
        v_ref[...] = jnp.exp2(start)
        m_ref[...] = jnp.broadcast_to(top, (width, lanes))

        def first_chunk(c, acc):
            at = pl.ds(pl.multiple_of(c * lanes, lanes), lanes)
            e = jnp.exp2(e_ref[i, :, at] - m_ref[...])
            e_ref[i, :, at] = e
            inv = 1.0 / (1.0 + jnp.sum(e * v_ref[...], axis=0, keepdims=True))
            return acc + e * inv

        def next_chunk(c, acc):
            at = pl.ds(pl.multiple_of(c * lanes, lanes), lanes)
            e = e_ref[i, :, at]
            inv = 1.0 / (1.0 + jnp.sum(e * v_ref[...], axis=0, keepdims=True))
            return acc + e * inv

        def evaluate(turn, share):
            acc = lax.fori_loop(
                0, chunks, next_chunk, jnp.zeros((width, lanes), F32), unroll=U_NEXT
            )
            share = jnp.sum(acc, axis=1, keepdims=True) * (1.0 / total)
            v_ref[...] = obs_col / share
            return share

        acc = lax.fori_loop(
            0, chunks, first_chunk, jnp.zeros((width, lanes), F32), unroll=U_FIRST
        )
        share = jnp.sum(acc, axis=1, keepdims=True) * (1.0 / total)
        v_ref[...] = obs_col / share
        share = lax.fori_loop(1, ITERS, evaluate, share)
        mean = jnp.log(obs_col) - jnp.log(share) - top * LN2

        def last_chunk(c, acc):
            at = pl.ds(pl.multiple_of(c * lanes, lanes), lanes)
            ve = e_ref[i, :, at] * v_ref[...]
            inv = 1.0 / (1.0 + jnp.sum(ve, axis=0, keepdims=True))
            root = root_ref[0:1, at]
            q = ve * (inv * root)
            high = q.astype(BF16)
            q_ref[0:width, at] = high
            q_ref[width:2 * width, at] = (q - high.astype(F32)).astype(BF16)
            return acc + q * root

        own = lax.fori_loop(0, chunks, last_chunk, jnp.zeros((width, lanes), F32), unroll=U_LAST)
        own = jnp.sum(own, axis=1, keepdims=True)
        both = lax.dot_general(
            q_ref[...], q_ref[...], (((1,), (1,)), ((), ())), preferred_element_type=F32
        )
        cross = both[0:width, 0:width] + (both[0:width, width:] + both[width:, 0:width])
        same = f_ref[i] == firms_ref[pl.ds(m, 1), :].astype(F32)
        n_ref[i] = jnp.where(same, eye * own - cross, 0.0) * (1.0 / total)
        return jnp.where(col_i == i, mean, finals)

    finals = lax.fori_loop(0, half, market, jnp.zeros((width, width), F32))
    util_ref[...] = finals.T[0:half, :]

    scales, c_rows, c_cols, y_rows, y_cols = [], [], [], [], []
    for i in range(half):
        jac = n_ref[i]
        diag = jac * eye
        s_row = lax.rsqrt(jnp.sum(diag, axis=0, keepdims=True))
        s_col = lax.rsqrt(jnp.sum(diag, axis=1, keepdims=True))
        n_ref[i] = eye - s_col * jac * s_row
        scales.append(s_row)
        c_rows.append(s_row * obs_rows[i])
        c_cols.append(s_col * b_ref[i, :, 0:1])
    y_rows = tuple(c_rows)

    def sweep(_, ys):
        out = []
        for i in range(half):
            y_col = c_cols[i] + jnp.sum(n_ref[i] * ys[i], axis=1, keepdims=True)
            out.append(c_rows[i] + jnp.sum(n_ref[i] * y_col, axis=0, keepdims=True))
        return tuple(out)

    y_rows = lax.fori_loop(0, SWEEPS, sweep, y_rows)
    rests = []
    for i in range(half):
        n_col = jnp.sum(n_ref[i] * y_rows[i], axis=1, keepdims=True)
        n_row = jnp.sum(eye * n_col, axis=0, keepdims=True)
        rests.append(c_rows[i] + n_row - y_rows[i])

    def size_of(vectors, against):
        worst = jnp.zeros((1, 1), F32)
        for i in range(half):
            top = jnp.max(jnp.abs(vectors[i]), axis=1, keepdims=True)
            worst = jnp.maximum(worst, top / jnp.max(jnp.abs(against[i]), axis=1, keepdims=True))
        return jnp.max(worst)

    def again(state):
        return jnp.logical_and(state[0] < DOUBLINGS, state[1] > TOL)

    def double(state):
        step, _, errors = state
        added, fresh = [], []
        for i in range(half):
            power = n_ref[i]
            eight = jnp.broadcast_to(errors[i], (8, width))
            more = jnp.dot(eight, power, precision=HIGH, preferred_element_type=F32)[0:1, :]
            added.append(more)
            fresh.append(errors[i] + more)
            n_ref[i] = jnp.dot(power, power, precision=HIGH, preferred_element_type=F32)
        return step + 1, size_of(added, y_rows), tuple(fresh)

    state = lax.while_loop(again, double, (0, size_of(rests, y_rows), tuple(rests)))
    out_row = lax.broadcasted_iota(jnp.int32, placed_ref.shape, 0)
    placed = jnp.zeros(placed_ref.shape, F32)
    for i in range(half):
        x = scales[i] * (y_rows[i] + state[2][i])
        mine = steps_ref[first + i]
        rank = 0
        for other in range(here):
            hit = jnp.logical_and(steps_ref[other] == mine, other < first + i)
            rank = rank + hit.astype(jnp.int32)
        upper = (rank >= CAPC).astype(jnp.int32)
        at = upper * (W * CAPC) + mine * CAPC + (rank - upper * CAPC)
        placed = jnp.where(out_row == at, x, placed)
    placed_ref[...] = placed


def solve_markets(coefs, params, steps, chars, taste, other, prices, obs, firms):
    terms, here, width = chars.shape
    half = here // 2
    total = 2 * taste.shape[2]
    smem = pl.BlockSpec(memory_space=pltpu.SMEM)
    vmem = pl.BlockSpec(memory_space=pltpu.VMEM)
    padded = -(-(terms + 1) // 8) * 8
    return pl.pallas_call(
        market_kernel,
        out_shape=(
            jax.ShapeDtypeStruct((half, width), F32),
            jax.ShapeDtypeStruct((2 * W * CAPC, width), F32),
        ),
        in_specs=[smem] * 3 + [vmem] * 6,
        out_specs=(vmem, vmem),
        scratch_shapes=[
            pltpu.VMEM((half, width, total), F32),
            pltpu.VMEM((2 * width, total), BF16),
            pltpu.VMEM((padded, width), F32),
            pltpu.VMEM((padded, total), F32),
            pltpu.VMEM((6 * padded, total), BF16),
            pltpu.VMEM((8, total), F32),
            pltpu.VMEM((width, 128), F32),
            pltpu.VMEM((half, width, width), F32),
            pltpu.VMEM((width, 128), F32),
            pltpu.VMEM((half, width, 128), F32),
            pltpu.VMEM((half, width, 128), F32),
            pltpu.VMEM((8, total), F32),
        ],
        name="markets",
    )(coefs, params, steps, chars, taste, other, prices, obs, firms)


def route_kernel(markets, placed_ref, out_ref, got_ref, send_sem, recv_sem):
    core = lax.axis_index("draw")
    me = lax.axis_index("mkt")
    pairs = [(w, flip) for w in range(W) for flip in range(2) if (w, flip) != (0, 0)]
    barrier = pltpu.get_barrier_semaphore()

    def peer(step, flip):
        to_core = core if flip == 0 else 1 - core
        return {"mkt": lax.rem(me + step + markets, markets), "draw": to_core}

    for w, flip in pairs:
        pl.semaphore_signal(barrier, inc=1, device_id=peer(-w, flip), device_id_type=MESH)
    pl.semaphore_wait(barrier, len(pairs))
    copies = []
    for w, flip in pairs:
        to_core = core if flip == 0 else 1 - core
        copy = pltpu.make_async_remote_copy(
            src_ref=placed_ref.at[to_core, w],
            dst_ref=got_ref.at[flip, w],
            send_sem=send_sem.at[flip, w],
            recv_sem=recv_sem.at[flip, w],
            device_id=peer(w, flip),
            device_id_type=MESH,
        )
        copy.start()
        copies.append(copy)
    for copy in copies:
        copy.wait()
    out_ref[0, 0] = placed_ref[core, 0] + got_ref[1, 0]
    for w in range(1, W):
        out_ref[0, w] = got_ref[0, w] + got_ref[1, w]


def route(markets, placed):
    width = placed.shape[-1]
    vmem = pl.BlockSpec(memory_space=pltpu.VMEM)
    return pl.pallas_call(
        functools.partial(route_kernel, markets),
        out_shape=jax.ShapeDtypeStruct((1, W, CAPC, width), F32),
        in_specs=[vmem],
        out_specs=vmem,
        scratch_shapes=[
            pltpu.VMEM((2, W, CAPC, width), F32),
            pltpu.SemaphoreType.DMA((2, W)),
            pltpu.SemaphoreType.DMA((2, W)),
        ],
        compiler_params=pltpu.CompilerParams(collective_id=1, has_side_effects=True),
        name="route",
    )(placed.reshape(2, W, CAPC, width))


def body(
    markets,
    characters, taste_draws, prices, obs_shares, firm_ids, owner_step, spread_coefs, price_params,
):
    characters = jnp.swapaxes(characters, 0, 1)
    taste_draws = jnp.swapaxes(taste_draws, 0, 1)
    other = exchange(taste_draws)
    mean_util, placed = solve_markets(
        spread_coefs, price_params, owner_step[:, 0], characters, taste_draws, other,
        prices, obs_shares, firm_ids,
    )
    return mean_util, route(markets, placed)


def solution(mesh):
    placed = (
        P(("parts", "mkt"), None, None),
        P(("parts", "mkt"), None, "draw"),
        P(("parts", "mkt"), None),
        P(("parts", "mkt"), None),
        P(("parts", "mkt"), None),
        P(("parts", "mkt"), None),
        P(),
        P(),
    )
    return jax.shard_map(
        functools.partial(body, mesh.shape["mkt"]),
        mesh=mesh,
        in_specs=placed,
        out_specs=(P(("parts", "mkt", "draw"), None), P(("parts", "mkt"), None, "draw", None)),
        check_vma=False,
    )
```

```python
import functools

import jax
import jax.numpy as jnp
from jax import lax
from jax.experimental import pallas as pl
from jax.experimental.pallas import tpu as pltpu
from jax.sharding import PartitionSpec as P

ITERS = 4
CAPC = 2
W = 8
LOG2E = 1.4426950408889634
LN2 = 0.6931471805599453
SWEEPS = 6
U_SPREAD = 8
U_FIRST = 32
U_NEXT = 32
U_LAST = 32
DOUBLINGS = 26
TOL = 3e-7
MESH = pl.DeviceIdType.MESH
HIGH = lax.Precision.HIGHEST
F32 = jnp.float32
BF16 = jnp.bfloat16


def exchange_kernel(taste_ref, out_ref, send_sem, recv_sem):
    core = lax.axis_index("draw")
    barrier = pltpu.get_barrier_semaphore()
    pl.semaphore_signal(barrier, inc=1, device_id={"draw": 1 - core}, device_id_type=MESH)
    pl.semaphore_wait(barrier, 1)
    copy = pltpu.make_async_remote_copy(
        src_ref=taste_ref,
        dst_ref=out_ref,
        send_sem=send_sem,
        recv_sem=recv_sem,
        device_id={"draw": 1 - core},
        device_id_type=MESH,
    )
    copy.start()
    copy.wait()


def exchange(taste_draws):
    return pl.pallas_call(
        exchange_kernel,
        out_shape=jax.ShapeDtypeStruct(taste_draws.shape, F32),
        in_specs=[pl.BlockSpec(memory_space=pl.ANY)],
        out_specs=pl.BlockSpec(memory_space=pl.ANY),
        scratch_shapes=[pltpu.SemaphoreType.DMA, pltpu.SemaphoreType.DMA],
        compiler_params=pltpu.CompilerParams(collective_id=0, has_side_effects=True),
        name="exchange",
    )(taste_draws)


def split3(value):
    high = value.astype(BF16).astype(F32)
    rest = value - high
    middle = rest.astype(BF16).astype(F32)
    return high, middle, rest - middle


def market_kernel(
    coef_ref, params_ref, steps_ref, chars_ref, taste_ref, other_ref, prices_ref, obs_ref,
    firms_ref, util_ref, placed_ref,
    e_ref, q_ref, left_ref, right_ref, stack_ref, root_ref, v_ref, n_ref, m_ref, b_ref, f_ref,
    inv_ref,
):
    core = lax.axis_index("draw")
    terms, here, width = chars_ref.shape
    half = here // 2
    part = taste_ref.shape[2]
    total = 2 * part
    lanes = 128
    chunks = total // lanes
    first = core * half

    row_i = lax.broadcasted_iota(jnp.int32, (width, width), 0)
    col_i = lax.broadcasted_iota(jnp.int32, (width, width), 1)
    eye = (row_i == col_i).astype(F32)

    obs_rows = [obs_ref[pl.ds(first + i, 1), :] for i in range(half)]
    rows = jnp.zeros((width, width), F32)
    for i in range(half):
        rows = jnp.where(row_i == i, obs_rows[i], rows)
        firm_row = firms_ref[pl.ds(first + i, 1), :].astype(F32)
        rows = jnp.where(row_i == half + i, firm_row, rows)
    cols = rows.T
    for i in range(half):
        b_ref[i] = jnp.broadcast_to(cols[:, i:i + 1], (width, lanes))
        f_ref[i] = jnp.broadcast_to(cols[:, half + i:half + i + 1], (width, lanes))
    left_ref[...] = jnp.zeros_like(left_ref)
    right_ref[...] = jnp.zeros_like(right_ref)

    def market(i, finals):
        m = first + i
        obs_row = obs_ref[pl.ds(m, 1), :]
        obs_col = b_ref[i]
        for k in range(terms):
            left_ref[k:k + 1, :] = chars_ref[k, pl.ds(m, 1), :] * coef_ref[k] * LOG2E
        left_ref[terms:terms + 1, :] = prices_ref[pl.ds(m, 1), :] * (-LOG2E)
        lh, lm, ll = split3(left_ref[...])
        left = jnp.concatenate([lh, lh, lm, lm, lh, ll], axis=0).T.astype(BF16)
        for h, source in enumerate((taste_ref, other_ref)):
            at = slice(h * part, (h + 1) * part)
            for k in range(terms):
                right_ref[k:k + 1, at] = source[k, pl.ds(m, 1), :]
            log_sens = (params_ref[0] + params_ref[1] * right_ref[0:1, at]) * LOG2E
            root = jnp.exp2(0.5 * log_sens)
            root_ref[0:1, at] = root
            right_ref[terms:terms + 1, at] = jnp.exp2(log_sens)
        xh, xm, xl = split3(right_ref[...])
        stack_ref[...] = jnp.concatenate([xh, xm, xh, xm, xl, xh], axis=0).astype(BF16)

        wide = 4 * lanes

        def spread_chunk(c, top):
            at = pl.ds(pl.multiple_of(c * wide, wide), wide)
            s = jnp.dot(left, stack_ref[:, at], preferred_element_type=F32)
            e_ref[i, :, at] = s
            for b in range(4):
                top = jnp.maximum(top, s[:, b * lanes:(b + 1) * lanes])
            return top

        top = lax.fori_loop(
            0, total // wide, spread_chunk, jnp.full((width, lanes), -jnp.inf, F32),
            unroll=U_SPREAD,
        )
        top = jnp.max(top, axis=1, keepdims=True)
        outside = 1.0 - jnp.sum(obs_row, axis=1, keepdims=True)
        start = (jnp.log(obs_col) - jnp.log(outside)) * LOG2E + top
        v_ref[...] = jnp.exp2(start)
        m_ref[...] = jnp.broadcast_to(top, (width, lanes))

        def first_chunk(c, acc):
            at = pl.ds(pl.multiple_of(c * lanes, lanes), lanes)
            e = jnp.exp2(e_ref[i, :, at] - m_ref[...])
            e_ref[i, :, at] = e
            inv = 1.0 / (1.0 + jnp.sum(e * v_ref[...], axis=0, keepdims=True))
            return acc + e * inv

        def next_chunk(c, acc):
            at = pl.ds(pl.multiple_of(c * lanes, lanes), lanes)
            e = e_ref[i, :, at]
            inv = 1.0 / (1.0 + jnp.sum(e * v_ref[...], axis=0, keepdims=True))
            return acc + e * inv

        def evaluate(turn, share):
            acc = lax.fori_loop(
                0, chunks, next_chunk, jnp.zeros((width, lanes), F32), unroll=U_NEXT
            )
            share = jnp.sum(acc, axis=1, keepdims=True) * (1.0 / total)
            v_ref[...] = obs_col / share
            return share

        acc = lax.fori_loop(
            0, chunks, first_chunk, jnp.zeros((width, lanes), F32), unroll=U_FIRST
        )
        share = jnp.sum(acc, axis=1, keepdims=True) * (1.0 / total)
        v_ref[...] = obs_col / share
        for turn in range(1, ITERS):
            share = evaluate(turn, share)
        mean = jnp.log(obs_col) - jnp.log(share) - top * LN2

        def last_chunk(c, acc):
            at = pl.ds(pl.multiple_of(c * lanes, lanes), lanes)
            ve = e_ref[i, :, at] * v_ref[...]
            inv = 1.0 / (1.0 + jnp.sum(ve, axis=0, keepdims=True))
            root = root_ref[0:1, at]
            q = ve * (inv * root)
            high = q.astype(BF16)
            q_ref[0:width, at] = high
            q_ref[width:2 * width, at] = (q - high.astype(F32)).astype(BF16)
            return acc + q * root

        own = lax.fori_loop(0, chunks, last_chunk, jnp.zeros((width, lanes), F32), unroll=U_LAST)
        own = jnp.sum(own, axis=1, keepdims=True)
        both = lax.dot_general(
            q_ref[...], q_ref[...], (((1,), (1,)), ((), ())), preferred_element_type=F32
        )
        cross = both[0:width, 0:width] + (both[0:width, width:] + both[width:, 0:width])
        same = f_ref[i] == firms_ref[pl.ds(m, 1), :].astype(F32)
        n_ref[i] = jnp.where(same, eye * own - cross, 0.0) * (1.0 / total)
        return jnp.where(col_i == i, mean, finals)

    finals = lax.fori_loop(0, half, market, jnp.zeros((width, width), F32))
    util_ref[...] = finals.T[0:half, :]

    scales, c_rows, c_cols, y_rows, y_cols = [], [], [], [], []
    for i in range(half):
        jac = n_ref[i]
        diag = jac * eye
        s_row = lax.rsqrt(jnp.sum(diag, axis=0, keepdims=True))
        s_col = lax.rsqrt(jnp.sum(diag, axis=1, keepdims=True))
        n_ref[i] = eye - s_col * jac * s_row
        scales.append(s_row)
        c_rows.append(s_row * obs_rows[i])
        c_cols.append(s_col * b_ref[i, :, 0:1])
    y_rows = tuple(c_rows)

    def sweep(_, ys):
        out = []
        for i in range(half):
            y_col = c_cols[i] + jnp.sum(n_ref[i] * ys[i], axis=1, keepdims=True)
            out.append(c_rows[i] + jnp.sum(n_ref[i] * y_col, axis=0, keepdims=True))
        return tuple(out)

    y_rows = lax.fori_loop(0, SWEEPS, sweep, y_rows)
    rests = []
    for i in range(half):
        n_col = jnp.sum(n_ref[i] * y_rows[i], axis=1, keepdims=True)
        n_row = jnp.sum(eye * n_col, axis=0, keepdims=True)
        rests.append(c_rows[i] + n_row - y_rows[i])

    def size_of(vectors, against):
        worst = jnp.zeros((1, 1), F32)
        for i in range(half):
            top = jnp.max(jnp.abs(vectors[i]), axis=1, keepdims=True)
            worst = jnp.maximum(worst, top / jnp.max(jnp.abs(against[i]), axis=1, keepdims=True))
        return jnp.max(worst)

    def again(state):
        return jnp.logical_and(state[0] < DOUBLINGS, state[1] > TOL)

    def double(state):
        step, _, errors = state
        added, fresh = [], []
        for i in range(half):
            power = n_ref[i]
            eight = jnp.broadcast_to(errors[i], (8, width))
            more = jnp.dot(eight, power, precision=HIGH, preferred_element_type=F32)[0:1, :]
            added.append(more)
            fresh.append(errors[i] + more)
            n_ref[i] = jnp.dot(power, power, precision=HIGH, preferred_element_type=F32)
        return step + 1, size_of(added, y_rows), tuple(fresh)

    state = lax.while_loop(again, double, (0, size_of(rests, y_rows), tuple(rests)))
    out_row = lax.broadcasted_iota(jnp.int32, placed_ref.shape, 0)
    placed = jnp.zeros(placed_ref.shape, F32)
    for i in range(half):
        x = scales[i] * (y_rows[i] + state[2][i])
        mine = steps_ref[first + i]
        rank = 0
        for other in range(here):
            hit = jnp.logical_and(steps_ref[other] == mine, other < first + i)
            rank = rank + hit.astype(jnp.int32)
        upper = (rank >= CAPC).astype(jnp.int32)
        at = upper * (W * CAPC) + mine * CAPC + (rank - upper * CAPC)
        placed = jnp.where(out_row == at, x, placed)
    placed_ref[...] = placed


def solve_markets(coefs, params, steps, chars, taste, other, prices, obs, firms):
    terms, here, width = chars.shape
    half = here // 2
    total = 2 * taste.shape[2]
    smem = pl.BlockSpec(memory_space=pltpu.SMEM)
    vmem = pl.BlockSpec(memory_space=pltpu.VMEM)
    padded = -(-(terms + 1) // 8) * 8
    return pl.pallas_call(
        market_kernel,
        out_shape=(
            jax.ShapeDtypeStruct((half, width), F32),
            jax.ShapeDtypeStruct((2 * W * CAPC, width), F32),
        ),
        in_specs=[smem] * 3 + [vmem] * 6,
        out_specs=(vmem, vmem),
        scratch_shapes=[
            pltpu.VMEM((half, width, total), F32),
            pltpu.VMEM((2 * width, total), BF16),
            pltpu.VMEM((padded, width), F32),
            pltpu.VMEM((padded, total), F32),
            pltpu.VMEM((6 * padded, total), BF16),
            pltpu.VMEM((8, total), F32),
            pltpu.VMEM((width, 128), F32),
            pltpu.VMEM((half, width, width), F32),
            pltpu.VMEM((width, 128), F32),
            pltpu.VMEM((half, width, 128), F32),
            pltpu.VMEM((half, width, 128), F32),
            pltpu.VMEM((8, total), F32),
        ],
        name="markets",
    )(coefs, params, steps, chars, taste, other, prices, obs, firms)


def route_kernel(markets, placed_ref, got_ref, send_sem, recv_sem):
    core = lax.axis_index("draw")
    me = lax.axis_index("mkt")
    pairs = [(w, flip) for w in range(W) for flip in range(2) if (w, flip) != (0, 0)]
    barrier = pltpu.get_barrier_semaphore()

    def peer(step, flip):
        to_core = core if flip == 0 else 1 - core
        return {"mkt": lax.rem(me + step + markets, markets), "draw": to_core}

    for w, flip in pairs:
        pl.semaphore_signal(barrier, inc=1, device_id=peer(-w, flip), device_id_type=MESH)
    keep = pltpu.make_async_copy(placed_ref.at[core, 0], got_ref.at[0, 0], send_sem.at[0, 0])
    keep.start()
    pl.semaphore_wait(barrier, len(pairs))
    copies = []
    for w, flip in pairs:
        to_core = core if flip == 0 else 1 - core
        copy = pltpu.make_async_remote_copy(
            src_ref=placed_ref.at[to_core, w],
            dst_ref=got_ref.at[flip, w],
            send_sem=send_sem.at[flip, w],
            recv_sem=recv_sem.at[flip, w],
            device_id=peer(w, flip),
            device_id_type=MESH,
        )
        copy.start()
        copies.append(copy)
    for copy in copies:
        copy.wait()
    keep.wait()


def route(markets, placed):
    width = placed.shape[-1]
    anywhere = pl.BlockSpec(memory_space=pl.ANY)
    return pl.pallas_call(
        functools.partial(route_kernel, markets),
        out_shape=jax.ShapeDtypeStruct((2, W, CAPC, width), F32),
        in_specs=[anywhere],
        out_specs=anywhere,
        scratch_shapes=[
            pltpu.SemaphoreType.DMA((2, W)),
            pltpu.SemaphoreType.DMA((2, W)),
        ],
        compiler_params=pltpu.CompilerParams(collective_id=1, has_side_effects=True),
        name="route",
    )(placed.reshape(2, W, CAPC, width))


def body(
    markets,
    characters, taste_draws, prices, obs_shares, firm_ids, owner_step, spread_coefs, price_params,
):
    characters = jnp.swapaxes(characters, 0, 1)
    taste_draws = jnp.swapaxes(taste_draws, 0, 1)
    other = exchange(taste_draws)
    mean_util, placed = solve_markets(
        spread_coefs, price_params, owner_step[:, 0], characters, taste_draws, other,
        prices, obs_shares, firm_ids,
    )
    got = route(markets, placed)
    return mean_util, (got[0] + got[1])[None]


def solution(mesh):
    placed = (
        P(("parts", "mkt"), None, None),
        P(("parts", "mkt"), None, "draw"),
        P(("parts", "mkt"), None),
        P(("parts", "mkt"), None),
        P(("parts", "mkt"), None),
        P(("parts", "mkt"), None),
        P(),
        P(),
    )
    return jax.shard_map(
        functools.partial(body, mesh.shape["mkt"]),
        mesh=mesh,
        in_specs=placed,
        out_specs=(P(("parts", "mkt", "draw"), None), P(("parts", "mkt"), None, "draw", None)),
        check_vma=False,
    )
```
